32 devices in a mesh: samp: 4 (over x, core), feat: 8 (over z, y).
Axes of the slice: x: 2, y: 2, z: 4, core: 2. Of those that a mesh axis runs over, the one named last changes fastest.
Arguments:
- design: float32 [4096, 65536], P('samp', 'feat'), may hold values from -0.09375 to 0.09375
- coefficients: float32 [192, 65536], P(None, 'feat'), may hold values from -3 to 3
- response: float32 [192, 4096], P(None, 'samp'), may hold values from -6 to 6
- active_set: int32 [192, 65536], P(None, 'feat'), may hold values 0 or 1
- lambda_path: float32 [192, 16], P('samp'), may hold values from 0.5 to 4
- lambda_index: int32 [192], P('samp'), may hold values from 1 to 15
Outputs:
- margins: float32 [192, 65536], P('samp', 'feat')
- peak_gradient: float32 [192], P('samp')
- violation: float32 [192], P('samp')
- screen_mass: float32 [192], P('samp')
The draws below stay inside these ranges and needn't reach their ends.
Inputs may be any that keep to these rules, and one draw needn't show every extreme that they name: `active_set`: 1 marks a feature in the response's active set, 0 one outside it. `lambda_index`: the current point on the response's path; the previous point is the one just below it.
All inputs are finite; a program needn't handle non-finite values. No bound on the sum of `active_set` on one device may be relied on, other than what follows from the above.
Results may differ from the reference program's by a relative error of at most 0.000073.
Values sent between devices are 32-bit elements; how exact they have to be, the bound alone decides.
A program may use at most 128 MiB of HBM per device.

```python
import math
import jax
import jax.numpy as jnp
from jax import lax

NF = 65536
R = 192
L = 16
NS = 4096


def plant(result, stream_key, smallest, largest):
    longest = result.shape.index(max(result.shape))
    spots = []
    for shift in (0, 1):
        where = [jax.random.randint(jax.random.fold_in(stream_key, axis), (), 0, length) for axis, length in enumerate(result.shape)]
        where[longest] = (where[longest] + shift) % result.shape[longest]
        spots.append(tuple(where))
    return result.at[spots[0]].set(smallest).at[spots[1]].set(largest)


def level_of(stream_key, dims, pieces, low, largest):
    gain = 1.0
    for position, parts in pieces:
        draws = jax.random.uniform(jax.random.fold_in(jax.random.fold_in(stream_key, 6), position), (parts,), jnp.float32, low / len(pieces), largest / len(pieces))
        gain = gain * jnp.repeat(jnp.exp(draws), dims[position] // parts).reshape((-1,) + (1,) * (len(dims) - 1 - position))
    return gain


def noise(stream_key, dims, deviation, reach, pieces=(), kind=jnp.bfloat16):
    factor_of = level_of(stream_key, dims, pieces, -0.22, 0.18) if pieces else 1.0
    entries = jax.random.normal(stream_key, dims, jnp.float32) * deviation * factor_of
    return jnp.minimum(jnp.maximum(entries, -reach), reach).astype(kind)


def setup_inputs(seed: int = 0) -> dict:
    key_list = jax.random.split(jax.random.key(seed), 7)
    design = noise(key_list[0], (NS, NF), (NS ** -0.5), 0.09375, ((0, 4), (1, 8)), jnp.float32)
    coefficients = noise(key_list[1], (R, NF), (2.0 * NS ** 0.5 / NF ** 0.5), 3.0, ((1, 8),), jnp.float32)
    response = noise(key_list[2], (R, NS), 1.0, 6.0, ((1, 4),), jnp.float32)
    active_set = plant((jax.random.randint(key_list[3], (R, NF), 0, 4) < 1).astype(jnp.int32), jax.random.fold_in(key_list[3], 1), 0, 1)
    lambda_path = jnp.clip(jnp.exp(math.log(4.0) - 2.0794415 * jax.random.uniform(key_list[4], (R, L), jnp.float32) ** level_of(key_list[4], (R, L), ((0, 4),), -0.2, 0.2)), 0.5, 4.0)
    lambda_index = plant(jax.random.randint(key_list[5], (R,), 1, L), jax.random.fold_in(key_list[5], 1), 1, L - 1).astype(jnp.int32)
    return dict(design=design, coefficients=coefficients, response=response, active_set=active_set, lambda_path=lambda_path, lambda_index=lambda_index)


def reference(design, coefficients, response, active_set, lambda_path, lambda_index):
    masked = coefficients * active_set.astype(jnp.float32)
    fitted = lax.dot_general(masked, design, (((1,), (1,)), ((), ())), precision=lax.Precision.HIGHEST, preferred_element_type=jnp.float32)
    residual = response - fitted
    gradient = jnp.dot(residual, design, precision=lax.Precision.HIGHEST, preferred_element_type=jnp.float32)
    positions = jnp.arange(lambda_path.shape[1], dtype=jnp.int32)
    picker_now = (positions[None, :] == lambda_index[:, None]).astype(jnp.float32)
    picker_before = (positions[None, :] == (lambda_index[:, None] - 1)).astype(jnp.float32)
    lambda_new = jnp.sum(lambda_path * picker_now, axis=1)
    lambda_old = jnp.sum(lambda_path * picker_before, axis=1)
    threshold = 2.0 * lambda_new - lambda_old
    magnitude = jnp.abs(gradient)
    margins = magnitude - threshold[:, None]
    peak_gradient = jnp.max(magnitude, axis=1)
    inactive = 1.0 - active_set.astype(jnp.float32)
    violation = jnp.sum(inactive * jnp.maximum(magnitude - lambda_new[:, None], 0.0), axis=1) / NF
    screen_mass = jnp.sum(jnp.maximum(margins, 0.0), axis=1) / NF
    return (margins, peak_gradient, violation, screen_mass)
```

```python
import functools

import jax
import jax.numpy as jnp
from jax import lax
from jax.experimental import pallas as pl
from jax.experimental.pallas import tpu as pltpu
from jax.sharding import PartitionSpec as P

MESH = pl.DeviceIdType.MESH
F32 = jnp.float32
BF16 = jnp.bfloat16
CHUNK = 256
TILE = 256
PIECE = 32
SLOTS = 4
CROWS = 48


def split(v):
    hi = v.astype(BF16)
    return hi, (v - hi.astype(F32)).astype(BF16)


def nt(a, b):
    return lax.dot_general(a, b, (((1,), (1,)), ((), ())), preferred_element_type=F32)


def kernel(
    cfg,
    design, coef, active, response, path, index,
    margins, stats_out,
    dh, dl, mm, stage, cst, ast, gb, crecv, xrecv, aown,
    part, yrecv, ysum, zrecv, full, resp, rr, sown, srecv,
    stage_sem, coef_sem, act_sem, resp_sem, aown_sem, out_sem,
    y_send, y_recv, z_send, z_recv, az_send, az_recv, ay_send, ay_recv,
    c_send, c_recv, x_send, x_recv, s_send, s_recv,
):
    S, F, A, B, X, R, rf, rp, rs, SL, FL = cfg
    Rp = F * rp
    C = SL // CHUNK
    T = FL // TILE
    KB = CHUNK // PIECE
    KW = FL // KB
    s = lax.axis_index("samp")
    f = lax.axis_index("feat")
    z = f // A
    y = f % A
    x = s // 2
    core = s % 2

    def padded(v):
        if rf == rp:
            return v
        fill = jnp.zeros((rp - rf, v.shape[1]), v.dtype)
        out = []
        for q in range(v.shape[0] // rf):
            out += [v[q * rf : (q + 1) * rf], fill]
        return jnp.concatenate(out, axis=0)

    barrier = pltpu.get_barrier_semaphore()
    peers = [(s, lax.rem(f + k, F)) for k in range(1, F)]
    peers += [(x * 2 + 1 - core, f)]
    peers += [(lax.rem(x + k, X) * 2 + core, f) for k in range(1, X)]
    for peer in peers:
        pl.semaphore_signal(barrier, inc=1, device_id=peer, device_id_type=MESH)

    half = FL // 2

    def coef_copies(i):
        rows = pl.ds((i // 2) * CROWS, CROWS)
        cols = pl.ds((i % 2) * half, half)
        return (
            pltpu.make_async_copy(coef.at[rows, cols], cst.at[i % 2], coef_sem.at[i % 2]),
            pltpu.make_async_copy(active.at[rows, cols], ast.at[i % 2], act_sem.at[i % 2]),
        )

    def piece_copy(p, slot):
        rows = pl.ds(pl.multiple_of(p * PIECE, PIECE), PIECE)
        return pltpu.make_async_copy(design.at[rows, :], stage.at[slot], stage_sem.at[slot])

    nc = 2 * R // CROWS
    NP = SL // PIECE
    for i in range(2):
        for cp in coef_copies(i):
            cp.start()
    for p in range(SLOTS):
        piece_copy(p, p).start()
    resp_copy = pltpu.make_async_copy(response, resp, resp_sem)
    for i in range(nc):
        for cp in coef_copies(i):
            cp.wait()
        m0 = (i // 2) * CROWS // rf * rp
        mr = CROWS // rf * rp
        step = 1024 if half % 1024 == 0 else half

        def mask_cols(j, carry, i=i, m0=m0, mr=mr, step=step):
            cols = pl.ds(pl.multiple_of(j * step, step), step)
            v = cst[i % 2, :, cols] * ast[i % 2, :, cols].astype(F32)
            hi, lo = split(padded(v))
            dst = pl.ds(pl.multiple_of((i % 2) * half + j * step, step), step)
            mm[m0 : m0 + mr, dst] = hi
            mm[Rp + m0 : Rp + m0 + mr, dst] = lo
            return carry

        lax.fori_loop(0, half // step, mask_cols, 0)
        if i + 2 < nc:
            for cp in coef_copies(i + 2):
                cp.start()
    resp_copy.start()
    own_first = pl.multiple_of(s * rs, 8)
    aown_copy = pltpu.make_async_copy(active.at[pl.ds(own_first, rs), :], aown, aown_sem)

    def split_piece(p):
        slot = lax.rem(p, SLOTS)
        piece_copy(p, slot).wait()
        rows = pl.ds(pl.multiple_of(p * PIECE, PIECE), PIECE)
        hi, lo = split(stage[slot])
        dh[rows, :] = hi
        dl[rows, :] = lo

    def next_piece(p):
        @pl.when(p + SLOTS < NP)
        def _():
            piece_copy(p + SLOTS, lax.rem(p, SLOTS)).start()

    def first_pieces(p, carry):
        split_piece(p)
        next_piece(p)
        return carry

    lax.fori_loop(0, KB, first_pieces, 0)
    pl.semaphore_wait(barrier, len(peers))

    def y_copy(c, k):
        to = lax.rem(y + k, A)
        return pltpu.make_async_remote_copy(
            part.at[c, to], yrecv.at[c, k - 1], y_send.at[c, k - 1], y_recv.at[c, k - 1],
            device_id=(s, z * A + to), device_id_type=MESH)

    def z_copy(c, k):
        to = lax.rem(z + k, B)
        return pltpu.make_async_remote_copy(
            ysum.at[c, to], zrecv.at[c, k - 1], z_send.at[c, k - 1], z_recv.at[c, k - 1],
            device_id=(s, to * A + y), device_id_type=MESH)

    def az_copy(c, k):
        to = lax.rem(z + k, B)
        return pltpu.make_async_remote_copy(
            full.at[c, y, z], full.at[c, y, z], az_send.at[c, k - 1], az_recv.at[c, k - 1],
            device_id=(s, to * A + y), device_id_type=MESH)

    def ay_copy(c, k):
        to = lax.rem(y + k, A)
        return pltpu.make_async_remote_copy(
            full.at[c, y], full.at[c, y], ay_send.at[c, k - 1], ay_recv.at[c, k - 1],
            device_id=(s, z * A + to), device_id_type=MESH)

    def stage1(c):
        for k in range(1, A):
            y_copy(c, k).start()

    def stage2(c):
        total = part[c, y]
        for k in range(1, A):
            y_copy(c, k).wait_recv()
            total = total + yrecv[c, k - 1]
        ysum[c] = total
        for k in range(1, B):
            z_copy(c, k).start()

    def stage3(c):
        total = ysum[c, z]
        for k in range(1, B):
            z_copy(c, k).wait_recv()
            total = total + zrecv[c, k - 1]
        full[c, y, z] = total
        for k in range(1, B):
            az_copy(c, k).start()

    def stage4(c):
        for k in range(1, B):
            az_copy(c, k).wait_recv()
        for k in range(1, A):
            ay_copy(c, k).start()

    def stage5(c):
        for k in range(1, A):
            ay_copy(c, k).wait_recv()
        cols = slice(c * CHUNK, (c + 1) * CHUNK)
        fitted = full[c].reshape(Rp, CHUNK)
        hi, lo = split(padded(resp[:, cols]) - fitted)
        rr[0:Rp, cols] = hi
        rr[Rp : 2 * Rp, cols] = lo

    stages = (stage1, stage2, stage3, stage4, stage5)
    for c in range(C + 4):
        if c < C:
            def fit(j, acc, c=c):
                cols = pl.ds(pl.multiple_of(j * KW, KW), KW)
                rows = slice(c * CHUNK, (c + 1) * CHUNK)
                if c + 1 < C:
                    split_piece((c + 1) * KB + j)
                both = nt(mm[:, cols], dh[rows, cols])
                small = nt(mm[0:Rp, cols], dl[rows, cols])
                if c + 1 < C:
                    next_piece((c + 1) * KB + j)
                return acc + (both[0:Rp] + (both[Rp:] + small))

            acc = lax.fori_loop(0, KB, fit, jnp.zeros((Rp, CHUNK), F32))
            part[c] = acc.reshape(A, B, rp, CHUNK)
        if c == C - 1:
            aown_copy.start()
            resp_copy.wait()
        for n, g in enumerate(stages):
            if 0 <= c - n < C:
                g(c - n)

    def c_copy(t):
        return pltpu.make_async_remote_copy(
            gb.at[t, 1 - core], crecv.at[t], c_send.at[t], c_recv.at[t],
            device_id=(x * 2 + 1 - core, f), device_id_type=MESH)

    def x_copy(t, k):
        to = lax.rem(x + k, X)
        return pltpu.make_async_remote_copy(
            gb.at[t, core, to], xrecv.at[t, k - 1], x_send.at[t, k - 1], x_recv.at[t, k - 1],
            device_id=(to * 2 + core, f), device_id_type=MESH)

    def forward(t):
        c_copy(t).wait_recv()
        gb[t, core] = gb[t, core] + crecv[t]
        for k in range(1, X):
            x_copy(t, k).start()

    def grad(t, carry):
        cols = pl.ds(pl.multiple_of(t * TILE, TILE), TILE)
        both = jnp.dot(rr[...], dh[:, cols], preferred_element_type=F32)
        small = jnp.dot(rr[0:Rp, :], dl[:, cols], preferred_element_type=F32)
        g = both[0:Rp] + (both[Rp:] + small)
        if rf == rp:
            for o in range(S):
                gb[t, o % 2, o // 2] = g[o * rs : (o + 1) * rs]
        else:
            for q in range(F):
                o, r0 = q * rf // rs, q * rf % rs
                gb[t, o % 2, o // 2, r0 : r0 + rf, :] = g[q * rp : q * rp + rf]
        c_copy(t).start()

        @pl.when(t > 0)
        def _():
            forward(t - 1)

        return carry

    lax.fori_loop(0, T, grad, 0)
    forward(T - 1)
    aown_copy.wait()

    where = index[...]
    spots = lax.broadcasted_iota(jnp.int32, path.shape, 1)
    lam_new = jnp.sum(jnp.where(spots == where, path[...], 0.0), axis=1, keepdims=True)
    lam_old = jnp.sum(jnp.where(spots == where - 1, path[...], 0.0), axis=1, keepdims=True)
    threshold = 2.0 * lam_new - lam_old

    def out_copy(t):
        cols = pl.ds(pl.multiple_of(t * TILE, TILE), TILE)
        return pltpu.make_async_copy(xrecv.at[t, 0], margins.at[:, cols], out_sem.at[t])

    def finish(t, carry):
        peak, viol, mass = carry
        total = gb[t, core, x]
        for k in range(1, X):
            x_copy(t, k).wait_recv()
            total = total + xrecv[t, k - 1]
        cols = pl.ds(pl.multiple_of(t * TILE, TILE), TILE)
        mag = jnp.abs(total)
        mar = mag - threshold
        xrecv[t, 0] = mar
        out_copy(t).start()
        inactive = 1.0 - aown[:, cols].astype(F32)
        peak = jnp.maximum(peak, mag)
        viol = viol + inactive * jnp.maximum(mag - lam_new, 0.0)
        mass = mass + jnp.maximum(mar, 0.0)
        return peak, viol, mass

    zero = jnp.zeros((rs, TILE), F32)
    peak, viol, mass = lax.fori_loop(0, T, finish, (zero, zero, zero))
    lane = lax.broadcasted_iota(jnp.int32, (rs, 128), 1)
    peak = jnp.max(peak, axis=1, keepdims=True)
    viol = jnp.sum(viol, axis=1, keepdims=True)
    mass = jnp.sum(mass, axis=1, keepdims=True)
    mine = jnp.where(lane == 0, peak, jnp.where(lane == 1, viol, mass))
    sown[...] = mine

    def s_copy(k):
        return pltpu.make_async_remote_copy(
            sown, srecv.at[k - 1], s_send.at[k - 1], s_recv.at[k - 1],
            device_id=(s, lax.rem(f + k, F)), device_id_type=MESH)

    for k in range(1, F):
        s_copy(k).start()

    for c in range(C):
        for k in range(1, A):
            y_copy(c, k).wait_send()
            ay_copy(c, k).wait_send()
        for k in range(1, B):
            z_copy(c, k).wait_send()
            az_copy(c, k).wait_send()

    def drain(t, carry):
        c_copy(t).wait_send()
        for k in range(1, X):
            x_copy(t, k).wait_send()
        out_copy(t).wait()
        return carry

    lax.fori_loop(0, T, drain, 0)
    top, add = mine, mine
    for k in range(1, F):
        s_copy(k).wait_recv()
        top = jnp.maximum(top, srecv[k - 1])
        add = add + srecv[k - 1]
    stats_out[...] = jnp.where(lane == 0, top, add / (FL * F))
    for k in range(1, F):
        s_copy(k).wait_send()


def body(S, F, design, coefficients, response, active_set, lambda_path, lambda_index):
    SL, FL = design.shape
    R = coefficients.shape[0]
    rs = lambda_path.shape[0]
    A = 1
    while (2 * A) ** 2 <= F:
        A *= 2
    B = F // A
    X = S // 2
    rf = R // F
    rp = -(-rf // 8) * 8
    Rp = F * rp
    C, T = SL // CHUNK, FL // TILE
    cfg = (S, F, A, B, X, R, rf, rp, rs, SL, FL)
    hbm = pl.BlockSpec(memory_space=pl.ANY)
    vmem = pl.BlockSpec(memory_space=pltpu.VMEM)
    dma = pltpu.SemaphoreType.DMA
    margins, stats = pl.pallas_call(
        functools.partial(kernel, cfg),
        out_shape=(
            jax.ShapeDtypeStruct((rs, FL), F32),
            jax.ShapeDtypeStruct((rs, 128), F32),
        ),
        in_specs=[hbm, hbm, hbm, hbm, vmem, vmem],
        out_specs=(hbm, vmem),
        scratch_shapes=[
            pltpu.VMEM((SL, FL), BF16),
            pltpu.VMEM((SL, FL), BF16),
            pltpu.VMEM((2 * Rp, FL), BF16),
            pltpu.VMEM((SLOTS, PIECE, FL), F32),
            pltpu.VMEM((2, CROWS, FL // 2), F32),
            pltpu.VMEM((2, CROWS, FL // 2), jnp.int32),
            pltpu.VMEM((T, 2, X, rs, TILE), F32),
            pltpu.VMEM((T, X, rs, TILE), F32),
            pltpu.VMEM((T, max(X - 1, 1), rs, TILE), F32),
            pltpu.VMEM((rs, FL), jnp.int32),
            pltpu.VMEM((C, A, B, rp, CHUNK), F32),
            pltpu.VMEM((C, A - 1, B, rp, CHUNK), F32),
            pltpu.VMEM((C, B, rp, CHUNK), F32),
            pltpu.VMEM((C, B - 1, rp, CHUNK), F32),
            pltpu.VMEM((C, A, B, rp, CHUNK), F32),
            pltpu.VMEM((R, SL), F32),
            pltpu.VMEM((2 * Rp, SL), BF16),
            pltpu.VMEM((rs, 128), F32),
            pltpu.VMEM((F - 1, rs, 128), F32),
            dma((SLOTS,)), dma((2,)), dma((2,)), dma, dma, dma((T,)),
            dma((C, A - 1)), dma((C, A - 1)), dma((C, B - 1)), dma((C, B - 1)),
            dma((C, B - 1)), dma((C, B - 1)), dma((C, A - 1)), dma((C, A - 1)),
            dma((T,)), dma((T,)), dma((T, X - 1)), dma((T, X - 1)),
            dma((F - 1,)), dma((F - 1,)),
        ],
        compiler_params=pltpu.CompilerParams(
            collective_id=0, has_side_effects=True, vmem_limit_bytes=67043328
        ),
    )(
        design, coefficients, active_set, response, lambda_path,
        lambda_index.reshape(rs, 1),
    )
    return margins, stats[:, 0], stats[:, 1], stats[:, 2]


def solution(mesh):
    return jax.shard_map(
        functools.partial(body, mesh.shape["samp"], mesh.shape["feat"]),
        mesh=mesh,
        in_specs=(
            P("samp", "feat"),
            P(None, "feat"),
            P(None, "samp"),
            P(None, "feat"),
            P("samp", None),
            P("samp"),
        ),
        out_specs=(P("samp", "feat"), P("samp"), P("samp"), P("samp")),
        check_vma=False,
    )
```

```python
import functools

import jax
import jax.numpy as jnp
from jax import lax
from jax.experimental import pallas as pl
from jax.experimental.pallas import tpu as pltpu
from jax.sharding import PartitionSpec as P

MESH = pl.DeviceIdType.MESH
F32 = jnp.float32
BF16 = jnp.bfloat16
CHUNK = 256
WIDE = 128
STEPS = 4
TILE = 256
PIECE = 32
SLOTS = 4
CROWS = 48


def split(v):
    hi = v.astype(BF16)
    return hi, (v - hi.astype(F32)).astype(BF16)


def nt(a, b):
    return lax.dot_general(a, b, (((1,), (1,)), ((), ())), preferred_element_type=F32)


def kernel(
    cfg,
    design, coef, active, response, path, index,
    margins, stats_out,
    parts, mm, stage, cst, ast, gb, crecv, xrecv, aown, pathv, indexv,
    part, yrecv, ysum, zrecv, full, resp, rr, sown, srecv,
    stage_sem, coef_sem, act_sem, resp_sem, aown_sem, path_sem, index_sem, out_sem,
    y_send, y_recv, z_send, z_recv, az_send, az_recv, ay_send, ay_recv,
    c_send, c_recv, x_send, x_recv, s_send, s_recv,
):
    S, F, A, B, X, R, rf, rp, rs, SL, FL = cfg
    Rp = F * rp
    C = SL // CHUNK
    V = CHUNK // WIDE
    T = FL // TILE
    KB = CHUNK // PIECE
    KW = FL // STEPS
    PS = KB // STEPS
    dh, dl = parts[:C], parts[C:]
    s = lax.axis_index("samp")
    f = lax.axis_index("feat")
    z = f // A
    y = f % A
    x = s // 2
    core = s % 2

    def padded(v):
        if rf == rp:
            return v
        fill = jnp.zeros((rp - rf, v.shape[1]), v.dtype)
        out = []
        for q in range(v.shape[0] // rf):
            out += [v[q * rf : (q + 1) * rf], fill]
        return jnp.concatenate(out, axis=0)

    barrier = pltpu.get_barrier_semaphore()
    peers = [(s, lax.rem(f + k, F)) for k in range(1, F)]
    peers += [(x * 2 + 1 - core, f)]
    peers += [(lax.rem(x + k, X) * 2 + core, f) for k in range(1, X)]
    for peer in peers:
        pl.semaphore_signal(barrier, inc=1, device_id=peer, device_id_type=MESH)

    half = FL // 2

    def coef_copies(i):
        rows = pl.ds((i // 2) * CROWS, CROWS)
        cols = pl.ds((i % 2) * half, half)
        return (
            pltpu.make_async_copy(coef.at[rows, cols], cst.at[i % 2], coef_sem.at[i % 2]),
            pltpu.make_async_copy(active.at[rows, cols], ast.at[i % 2], act_sem.at[i % 2]),
        )

    def piece_copy(p, slot):
        rows = pl.ds(pl.multiple_of(p * PIECE, PIECE), PIECE)
        return pltpu.make_async_copy(design.at[rows, :], stage.at[slot], stage_sem.at[slot])

    nc = 2 * R // CROWS
    NP = SL // PIECE
    for i in range(2):
        for cp in coef_copies(i):
            cp.start()
    for p in range(SLOTS):
        piece_copy(p, p).start()
    resp_copy = pltpu.make_async_copy(response, resp, resp_sem)
    path_copy = pltpu.make_async_copy(path, pathv, path_sem)
    index_copy = pltpu.make_async_copy(index, indexv, index_sem)
    for i in range(nc):
        for cp in coef_copies(i):
            cp.wait()
        m0 = (i // 2) * CROWS // rf * rp
        mr = CROWS // rf * rp
        step = 1024 if half % 1024 == 0 else half

        def mask_cols(j, carry, i=i, m0=m0, mr=mr, step=step):
            cols = pl.ds(pl.multiple_of(j * step, step), step)
            v = cst[i % 2, :, cols] * ast[i % 2, :, cols].astype(F32)
            hi, lo = split(padded(v))
            dst = pl.ds(pl.multiple_of((i % 2) * half + j * step, step), step)
            mm[m0 : m0 + mr, dst] = hi
            mm[Rp + m0 : Rp + m0 + mr, dst] = lo
            return carry

        lax.fori_loop(0, half // step, mask_cols, 0)
        if i + 2 < nc:
            for cp in coef_copies(i + 2):
                cp.start()
    resp_copy.start()
    path_copy.start()
    index_copy.start()
    own_first = pl.multiple_of(s * rs, 8)
    aown_copy = pltpu.make_async_copy(active.at[pl.ds(own_first, rs), :], aown, aown_sem)

    def split_piece(c, j):
        p = c * KB + j
        slot = lax.rem(p, SLOTS)
        piece_copy(p, slot).wait()
        rows = pl.ds(pl.multiple_of(j * PIECE, PIECE), PIECE)
        hi, lo = split(stage[slot])
        dh[c][rows, :] = hi
        dl[c][rows, :] = lo

    def next_piece(p):
        @pl.when(p + SLOTS < NP)
        def _():
            piece_copy(p + SLOTS, lax.rem(p, SLOTS)).start()

    def first_pieces(p, carry):
        split_piece(0, p)
        next_piece(p)
        return carry

    lax.fori_loop(0, KB, first_pieces, 0)
    pl.semaphore_wait(barrier, len(peers))

    def y_copy(c, k):
        to = lax.rem(y + k, A)
        return pltpu.make_async_remote_copy(
            part.at[c, to], yrecv.at[c, k - 1], y_send.at[c, k - 1], y_recv.at[c, k - 1],
            device_id=(s, z * A + to), device_id_type=MESH)

    def z_copy(c, k):
        to = lax.rem(z + k, B)
        return pltpu.make_async_remote_copy(
            ysum.at[c, to], zrecv.at[c, k - 1], z_send.at[c, k - 1], z_recv.at[c, k - 1],
            device_id=(s, to * A + y), device_id_type=MESH)

    def az_copy(c, k):
        to = lax.rem(z + k, B)
        return pltpu.make_async_remote_copy(
            full.at[c, y, z], full.at[c, y, z], az_send.at[c, k - 1], az_recv.at[c, k - 1],
            device_id=(s, to * A + y), device_id_type=MESH)

    def ay_copy(c, k):
        to = lax.rem(y + k, A)
        return pltpu.make_async_remote_copy(
            full.at[c, y], full.at[c, y], ay_send.at[c, k - 1], ay_recv.at[c, k - 1],
            device_id=(s, z * A + to), device_id_type=MESH)

    def stage1(c):
        for k in range(1, A):
            y_copy(c, k).start()

    def stage2(c):
        total = part[c, y]
        for k in range(1, A):
            y_copy(c, k).wait_recv()
            total = total + yrecv[c, k - 1]
        ysum[c] = total
        for k in range(1, B):
            z_copy(c, k).start()

    def stage3(c):
        total = ysum[c, z]
        for k in range(1, B):
            z_copy(c, k).wait_recv()
            total = total + zrecv[c, k - 1]
        full[c, y, z] = total
        for k in range(1, B):
            az_copy(c, k).start()

    def stage4(c):
        for k in range(1, B):
            az_copy(c, k).wait_recv()
        for k in range(1, A):
            ay_copy(c, k).start()

    def stage5(c):
        for k in range(1, A):
            ay_copy(c, k).wait_recv()
        cols = slice(c * WIDE, (c + 1) * WIDE)
        fitted = full[c].reshape(Rp, WIDE)
        hi, lo = split(padded(resp[:, cols]) - fitted)
        rr[0:Rp, cols] = hi
        rr[Rp : 2 * Rp, cols] = lo

    stages = (stage1, stage2, stage3, stage4, stage5)
    for c in range(C + 4):
        if c < C:
            def fit(j, acc, c=c):
                cols = pl.ds(pl.multiple_of(j * KW, KW), KW)
                if c + 1 < C:
                    for i in range(PS):
                        split_piece(c + 1, j * PS + i)
                both = nt(mm[:, cols], dh[c][:, cols])
                small = nt(mm[0:Rp, cols], dl[c][:, cols])
                if c + 1 < C:
                    for i in range(PS):
                        next_piece((c + 1) * KB + j * PS + i)
                return acc + (both[0:Rp] + (both[Rp:] + small))

            acc = lax.fori_loop(0, STEPS, fit, jnp.zeros((Rp, CHUNK), F32))
            for v in range(V):
                part[c * V + v] = acc[:, v * WIDE : (v + 1) * WIDE].reshape(A, B, rp, WIDE)
        if c == C - 1:
            aown_copy.start()
            resp_copy.wait()
        for n, g in enumerate(stages):
            if 0 <= c - n < C:
                for v in range(V):
                    g((c - n) * V + v)

    def c_copy(t):
        return pltpu.make_async_remote_copy(
            gb.at[t, 1 - core], crecv.at[t], c_send.at[t], c_recv.at[t],
            device_id=(x * 2 + 1 - core, f), device_id_type=MESH)

    def x_copy(t, k):
        to = lax.rem(x + k, X)
        return pltpu.make_async_remote_copy(
            gb.at[t, core, to], xrecv.at[t, k - 1], x_send.at[t, k - 1], x_recv.at[t, k - 1],
            device_id=(to * 2 + core, f), device_id_type=MESH)

    def forward(t):
        c_copy(t).wait_recv()
        gb[t, core] = gb[t, core] + crecv[t]
        for k in range(1, X):
            x_copy(t, k).start()

    def grad(t, carry):
        cols = pl.ds(pl.multiple_of(t * TILE, TILE), TILE)
        both = jnp.zeros((2 * Rp, TILE), F32)
        small = jnp.zeros((Rp, TILE), F32)
        for c in range(C):
            ks = slice(c * CHUNK, (c + 1) * CHUNK)
            both += jnp.dot(rr[:, ks], dh[c][:, cols], preferred_element_type=F32)
            small += jnp.dot(rr[0:Rp, ks], dl[c][:, cols], preferred_element_type=F32)
        g = both[0:Rp] + (both[Rp:] + small)
        if rf == rp:
            for o in range(S):
                gb[t, o % 2, o // 2] = g[o * rs : (o + 1) * rs]
        else:
            for q in range(F):
                o, r0 = q * rf // rs, q * rf % rs
                gb[t, o % 2, o // 2, r0 : r0 + rf, :] = g[q * rp : q * rp + rf]
        c_copy(t).start()

        @pl.when(t > 0)
        def _():
            forward(t - 1)

        return carry

    lax.fori_loop(0, T, grad, 0)
    forward(T - 1)
    aown_copy.wait()

    path_copy.wait()
    index_copy.wait()
    down = lax.broadcasted_iota(jnp.int32, (rs, rs), 0)
    across = lax.broadcasted_iota(jnp.int32, (rs, rs), 1)
    where = jnp.sum(jnp.where(down == across, indexv[...], 0), axis=1, keepdims=True)
    spots = lax.broadcasted_iota(jnp.int32, path.shape, 1)
    lam_new = jnp.sum(jnp.where(spots == where, pathv[...], 0.0), axis=1, keepdims=True)
    lam_old = jnp.sum(jnp.where(spots == where - 1, pathv[...], 0.0), axis=1, keepdims=True)
    threshold = 2.0 * lam_new - lam_old

    def out_copy(t):
        cols = pl.ds(pl.multiple_of(t * TILE, TILE), TILE)
        return pltpu.make_async_copy(xrecv.at[t, 0], margins.at[:, cols], out_sem.at[t])

    def finish(t, carry):
        peak, viol, mass = carry
        total = gb[t, core, x]
        for k in range(1, X):
            x_copy(t, k).wait_recv()
            total = total + xrecv[t, k - 1]
        cols = pl.ds(pl.multiple_of(t * TILE, TILE), TILE)
        mag = jnp.abs(total)
        mar = mag - threshold
        xrecv[t, 0] = mar
        out_copy(t).start()
        inactive = 1.0 - aown[:, cols].astype(F32)
        peak = jnp.maximum(peak, mag)
        viol = viol + inactive * jnp.maximum(mag - lam_new, 0.0)
        mass = mass + jnp.maximum(mar, 0.0)
        return peak, viol, mass

    zero = jnp.zeros((rs, TILE), F32)
    peak, viol, mass = lax.fori_loop(0, T, finish, (zero, zero, zero))
    lane = lax.broadcasted_iota(jnp.int32, (rs, 128), 1)
    peak = jnp.max(peak, axis=1, keepdims=True)
    viol = jnp.sum(viol, axis=1, keepdims=True)
    mass = jnp.sum(mass, axis=1, keepdims=True)
    mine = jnp.where(lane == 0, peak, jnp.where(lane == 1, viol, mass))
    sown[...] = mine

    def s_copy(k):
        return pltpu.make_async_remote_copy(
            sown, srecv.at[k - 1], s_send.at[k - 1], s_recv.at[k - 1],
            device_id=(s, lax.rem(f + k, F)), device_id_type=MESH)

    for k in range(1, F):
        s_copy(k).start()

    for c in range(C * V):
        for k in range(1, A):
            y_copy(c, k).wait_send()
            ay_copy(c, k).wait_send()
        for k in range(1, B):
            z_copy(c, k).wait_send()
            az_copy(c, k).wait_send()

    def drain(t, carry):
        c_copy(t).wait_send()
        for k in range(1, X):
            x_copy(t, k).wait_send()
        out_copy(t).wait()
        return carry

    lax.fori_loop(0, T, drain, 0)
    top, add = mine, mine
    for k in range(1, F):
        s_copy(k).wait_recv()
        top = jnp.maximum(top, srecv[k - 1])
        add = add + srecv[k - 1]
    stats_out[...] = jnp.where(lane == 0, top, add / (FL * F))
    for k in range(1, F):
        s_copy(k).wait_send()


def body(S, F, design, coefficients, response, active_set, lambda_path, lambda_index):
    SL, FL = design.shape
    R = coefficients.shape[0]
    rs = lambda_path.shape[0]
    A = 1
    while (2 * A) ** 2 <= F:
        A *= 2
    B = F // A
    X = S // 2
    rf = R // F
    rp = -(-rf // 8) * 8
    Rp = F * rp
    C, T, W = SL // CHUNK, FL // TILE, SL // WIDE
    cfg = (S, F, A, B, X, R, rf, rp, rs, SL, FL)
    hbm = pl.BlockSpec(memory_space=pl.ANY)
    vmem = pl.BlockSpec(memory_space=pltpu.VMEM)
    dma = pltpu.SemaphoreType.DMA
    margins, stats = pl.pallas_call(
        functools.partial(kernel, cfg),
        out_shape=(
            jax.ShapeDtypeStruct((rs, FL), F32),
            jax.ShapeDtypeStruct((rs, 128), F32),
        ),
        in_specs=[hbm] * 6,
        out_specs=(hbm, vmem),
        scratch_shapes=[
            [pltpu.VMEM((CHUNK, FL), BF16)] * (2 * C),
            pltpu.VMEM((2 * Rp, FL), BF16),
            pltpu.VMEM((SLOTS, PIECE, FL), F32),
            pltpu.VMEM((2, CROWS, FL // 2), F32),
            pltpu.VMEM((2, CROWS, FL // 2), jnp.int32),
            pltpu.VMEM((T, 2, X, rs, TILE), F32),
            pltpu.VMEM((T, X, rs, TILE), F32),
            pltpu.VMEM((T, max(X - 1, 1), rs, TILE), F32),
            pltpu.VMEM((rs, FL), jnp.int32),
            pltpu.VMEM(lambda_path.shape, F32),
            pltpu.VMEM((1, rs), jnp.int32),
            pltpu.VMEM((W, A, B, rp, WIDE), F32),
            pltpu.VMEM((W, A - 1, B, rp, WIDE), F32),
            pltpu.VMEM((W, B, rp, WIDE), F32),
            pltpu.VMEM((W, B - 1, rp, WIDE), F32),
            pltpu.VMEM((W, A, B, rp, WIDE), F32),
            pltpu.VMEM((R, SL), F32),
            pltpu.VMEM((2 * Rp, SL), BF16),
            pltpu.VMEM((rs, 128), F32),
            pltpu.VMEM((F - 1, rs, 128), F32),
            dma((SLOTS,)), dma((2,)), dma((2,)), dma, dma, dma, dma, dma((T,)),
            dma((W, A - 1)), dma((W, A - 1)), dma((W, B - 1)), dma((W, B - 1)),
            dma((W, B - 1)), dma((W, B - 1)), dma((W, A - 1)), dma((W, A - 1)),
            dma((T,)), dma((T,)), dma((T, X - 1)), dma((T, X - 1)),
            dma((F - 1,)), dma((F - 1,)),
        ],
        compiler_params=pltpu.CompilerParams(
            collective_id=0, has_side_effects=True, vmem_limit_bytes=67043328
        ),
    )(
        design, coefficients, active_set, response, lambda_path,
        lambda_index.reshape(1, rs),
    )
    return margins, stats[:, 0], stats[:, 1], stats[:, 2]


def solution(mesh):
    return jax.shard_map(
        functools.partial(body, mesh.shape["samp"], mesh.shape["feat"]),
        mesh=mesh,
        in_specs=(
            P("samp", "feat"),
            P(None, "feat"),
            P(None, "samp"),
            P(None, "feat"),
            P("samp", None),
            P("samp"),
        ),
        out_specs=(P("samp", "feat"), P("samp"), P("samp"), P("samp")),
        check_vma=False,
    )
```

```python
import functools

import jax
import jax.numpy as jnp
from jax import lax
from jax.experimental import pallas as pl
from jax.experimental.pallas import tpu as pltpu
from jax.sharding import PartitionSpec as P

MESH = pl.DeviceIdType.MESH
F32 = jnp.float32
BF16 = jnp.bfloat16
CHUNK = 256
WIDE = 128
STEPS = 4
TILE = 256
PIECE = 32
SLOTS = 4
CROWS = 48


def split(v):
    hi = v.astype(BF16)
    return hi, (v - hi.astype(F32)).astype(BF16)


def nt(a, b):
    return lax.dot_general(a, b, (((1,), (1,)), ((), ())), preferred_element_type=F32)


def kernel(
    cfg,
    design, coef, active, response, path, index,
    margins, stats_out,
    parts, mm, stage, cst, ast, gb, crecv, xrecv, aown, pathv, indexv,
    part, yrecv, ysum, zrecv, full, resp, rr, sown, srecv,
    stage_sem, coef_sem, act_sem, resp_sem, aown_sem, path_sem, index_sem, out_sem,
    y_send, y_recv, z_send, z_recv, az_send, az_recv, ay_send, ay_recv,
    c_send, c_recv, x_send, x_recv, s_send, s_recv,
):
    S, F, A, B, X, R, rf, rp, rs, SL, FL = cfg
    Rp = F * rp
    C = SL // CHUNK
    V = CHUNK // WIDE
    T = FL // TILE
    KB = CHUNK // PIECE
    KW = FL // STEPS
    PS = KB // STEPS
    dh, dl = parts[:C], parts[C:]
    s = lax.axis_index("samp")
    f = lax.axis_index("feat")
    z = f // A
    y = f % A
    x = s // 2
    core = s % 2

    def padded(v):
        if rf == rp:
            return v
        fill = jnp.zeros((rp - rf, v.shape[1]), v.dtype)
        out = []
        for q in range(v.shape[0] // rf):
            out += [v[q * rf : (q + 1) * rf], fill]
        return jnp.concatenate(out, axis=0)

    barrier = pltpu.get_barrier_semaphore()
    peers = [(s, lax.rem(f + k, F)) for k in range(1, F)]
    peers += [(x * 2 + 1 - core, f)]
    peers += [(lax.rem(x + k, X) * 2 + core, f) for k in range(1, X)]
    for peer in peers:
        pl.semaphore_signal(barrier, inc=1, device_id=peer, device_id_type=MESH)

    half = FL // 2

    def coef_copies(i):
        rows = pl.ds((i // 2) * CROWS, CROWS)
        cols = pl.ds((i % 2) * half, half)
        return (
            pltpu.make_async_copy(coef.at[rows, cols], cst.at[i % 2], coef_sem.at[i % 2]),
            pltpu.make_async_copy(active.at[rows, cols], ast.at[i % 2], act_sem.at[i % 2]),
        )

    def piece_copy(p, slot):
        rows = pl.ds(pl.multiple_of(p * PIECE, PIECE), PIECE)
        return pltpu.make_async_copy(design.at[rows, :], stage.at[slot], stage_sem.at[slot])

    nc = 2 * R // CROWS
    NP = SL // PIECE
    for i in range(2):
        for cp in coef_copies(i):
            cp.start()
    for p in range(SLOTS):
        piece_copy(p, p).start()
    resp_copy = pltpu.make_async_copy(response, resp, resp_sem)
    path_copy = pltpu.make_async_copy(path, pathv, path_sem)
    index_copy = pltpu.make_async_copy(index, indexv, index_sem)
    for i in range(nc):
        for cp in coef_copies(i):
            cp.wait()
        m0 = (i // 2) * CROWS // rf * rp
        mr = CROWS // rf * rp
        step = 1024 if half % 1024 == 0 else half

        def mask_cols(j, carry, i=i, m0=m0, mr=mr, step=step):
            cols = pl.ds(pl.multiple_of(j * step, step), step)
            v = cst[i % 2, :, cols] * ast[i % 2, :, cols].astype(F32)
            hi, lo = split(padded(v))
            dst = pl.ds(pl.multiple_of((i % 2) * half + j * step, step), step)
            mm[m0 : m0 + mr, dst] = hi
            mm[Rp + m0 : Rp + m0 + mr, dst] = lo
            return carry

        lax.fori_loop(0, half // step, mask_cols, 0)
        if i + 2 < nc:
            for cp in coef_copies(i + 2):
                cp.start()
    resp_copy.start()
    path_copy.start()
    index_copy.start()
    own_first = pl.multiple_of(s * rs, 8)
    aown_copy = pltpu.make_async_copy(active.at[pl.ds(own_first, rs), :], aown, aown_sem)

    def wait_piece(c, j):
        p = c * KB + j
        piece_copy(p, lax.rem(p, SLOTS)).wait()

    def split_piece(c, j):
        slot = lax.rem(c * KB + j, SLOTS)
        rows = pl.ds(pl.multiple_of(j * PIECE, PIECE), PIECE)
        hi, lo = split(stage[slot])
        dh[c][rows, :] = hi
        dl[c][rows, :] = lo

    def next_piece(p):
        @pl.when(p + SLOTS < NP)
        def _():
            piece_copy(p + SLOTS, lax.rem(p, SLOTS)).start()

    def first_pieces(p, carry):
        wait_piece(0, p)
        split_piece(0, p)
        next_piece(p)
        return carry

    lax.fori_loop(0, KB, first_pieces, 0)
    pl.semaphore_wait(barrier, len(peers))

    def y_copy(c, k):
        to = lax.rem(y + k, A)
        return pltpu.make_async_remote_copy(
            part.at[c, to], yrecv.at[c, k - 1], y_send.at[c, k - 1], y_recv.at[c, k - 1],
            device_id=(s, z * A + to), device_id_type=MESH)

    def z_copy(c, k):
        to = lax.rem(z + k, B)
        return pltpu.make_async_remote_copy(
            ysum.at[c, to], zrecv.at[c, k - 1], z_send.at[c, k - 1], z_recv.at[c, k - 1],
            device_id=(s, to * A + y), device_id_type=MESH)

    def az_copy(c, k):
        to = lax.rem(z + k, B)
        return pltpu.make_async_remote_copy(
            full.at[c, y, z], full.at[c, y, z], az_send.at[c, k - 1], az_recv.at[c, k - 1],
            device_id=(s, to * A + y), device_id_type=MESH)

    def ay_copy(c, k):
        to = lax.rem(y + k, A)
        return pltpu.make_async_remote_copy(
            full.at[c, y], full.at[c, y], ay_send.at[c, k - 1], ay_recv.at[c, k - 1],
            device_id=(s, z * A + to), device_id_type=MESH)

    def stage1(c):
        for k in range(1, A):
            y_copy(c, k).start()

    def stage2(c):
        total = part[c, y]
        for k in range(1, A):
            y_copy(c, k).wait_recv()
            total = total + yrecv[c, k - 1]
        ysum[c] = total
        for k in range(1, B):
            z_copy(c, k).start()

    def stage3(c):
        total = ysum[c, z]
        for k in range(1, B):
            z_copy(c, k).wait_recv()
            total = total + zrecv[c, k - 1]
        full[c, y, z] = total
        for k in range(1, B):
            az_copy(c, k).start()

    def stage4(c):
        for k in range(1, B):
            az_copy(c, k).wait_recv()
        for k in range(1, A):
            ay_copy(c, k).start()

    def stage5(c):
        for k in range(1, A):
            ay_copy(c, k).wait_recv()
        cols = slice(c * WIDE, (c + 1) * WIDE)
        fitted = full[c].reshape(Rp, WIDE)
        hi, lo = split(padded(resp[:, cols]) - fitted)
        rr[0:Rp, cols] = hi
        rr[Rp : 2 * Rp, cols] = lo

    stages = (stage1, stage2, stage3, stage4, stage5)
    for c in range(C + 4):
        if c < C:
            def fit(j, acc, c=c):
                cols = pl.ds(pl.multiple_of(j * KW, KW), KW)
                if c + 1 < C:
                    for i in range(PS):
                        wait_piece(c + 1, j * PS + i)
                both = nt(mm[:, cols], dh[c][:, cols])
                small = nt(mm[0:Rp, cols], dl[c][:, cols])
                if c + 1 < C:
                    for i in range(PS):
                        split_piece(c + 1, j * PS + i)
                    for i in range(PS):
                        next_piece((c + 1) * KB + j * PS + i)
                return acc + (both[0:Rp] + (both[Rp:] + small))

            acc = lax.fori_loop(0, STEPS, fit, jnp.zeros((Rp, CHUNK), F32))
            for v in range(V):
                part[c * V + v] = acc[:, v * WIDE : (v + 1) * WIDE].reshape(A, B, rp, WIDE)
        if c == C - 1:
            aown_copy.start()
            resp_copy.wait()
        for n, g in enumerate(stages):
            if 0 <= c - n < C:
                for v in range(V):
                    g((c - n) * V + v)

    def c_copy(t):
        return pltpu.make_async_remote_copy(
            gb.at[t, 1 - core], crecv.at[t], c_send.at[t], c_recv.at[t],
            device_id=(x * 2 + 1 - core, f), device_id_type=MESH)

    def x_copy(t, k):
        to = lax.rem(x + k, X)
        return pltpu.make_async_remote_copy(
            gb.at[t, core, to], xrecv.at[t, k - 1], x_send.at[t, k - 1], x_recv.at[t, k - 1],
            device_id=(to * 2 + core, f), device_id_type=MESH)

    def forward(t):
        c_copy(t).wait_recv()
        gb[t, core] = gb[t, core] + crecv[t]
        for k in range(1, X):
            x_copy(t, k).start()

    def grad(t, carry):
        cols = pl.ds(pl.multiple_of(t * TILE, TILE), TILE)
        both = jnp.zeros((2 * Rp, TILE), F32)
        small = jnp.zeros((Rp, TILE), F32)
        for c in range(C):
            ks = slice(c * CHUNK, (c + 1) * CHUNK)
            both += jnp.dot(rr[:, ks], dh[c][:, cols], preferred_element_type=F32)
            small += jnp.dot(rr[0:Rp, ks], dl[c][:, cols], preferred_element_type=F32)
        g = both[0:Rp] + (both[Rp:] + small)
        if rf == rp:
            for o in range(S):
                gb[t, o % 2, o // 2] = g[o * rs : (o + 1) * rs]
        else:
            for q in range(F):
                o, r0 = q * rf // rs, q * rf % rs
                gb[t, o % 2, o // 2, r0 : r0 + rf, :] = g[q * rp : q * rp + rf]
        c_copy(t).start()

        @pl.when(t > 0)
        def _():
            forward(t - 1)

        return carry

    lax.fori_loop(0, T, grad, 0)
    forward(T - 1)
    aown_copy.wait()

    path_copy.wait()
    index_copy.wait()
    down = lax.broadcasted_iota(jnp.int32, (rs, rs), 0)
    across = lax.broadcasted_iota(jnp.int32, (rs, rs), 1)
    where = jnp.sum(jnp.where(down == across, indexv[...], 0), axis=1, keepdims=True)
    spots = lax.broadcasted_iota(jnp.int32, path.shape, 1)
    lam_new = jnp.sum(jnp.where(spots == where, pathv[...], 0.0), axis=1, keepdims=True)
    lam_old = jnp.sum(jnp.where(spots == where - 1, pathv[...], 0.0), axis=1, keepdims=True)
    threshold = 2.0 * lam_new - lam_old

    def out_copy(t):
        cols = pl.ds(pl.multiple_of(t * TILE, TILE), TILE)
        return pltpu.make_async_copy(xrecv.at[t, 0], margins.at[:, cols], out_sem.at[t])

    def finish(t, carry):
        peak, viol, mass = carry
        total = gb[t, core, x]
        for k in range(1, X):
            x_copy(t, k).wait_recv()
            total = total + xrecv[t, k - 1]
        cols = pl.ds(pl.multiple_of(t * TILE, TILE), TILE)
        mag = jnp.abs(total)
        mar = mag - threshold
        xrecv[t, 0] = mar
        out_copy(t).start()
        inactive = 1.0 - aown[:, cols].astype(F32)
        peak = jnp.maximum(peak, mag)
        viol = viol + inactive * jnp.maximum(mag - lam_new, 0.0)
        mass = mass + jnp.maximum(mar, 0.0)
        return peak, viol, mass

    zero = jnp.zeros((rs, TILE), F32)
    peak, viol, mass = lax.fori_loop(0, T, finish, (zero, zero, zero))
    lane = lax.broadcasted_iota(jnp.int32, (rs, 128), 1)
    peak = jnp.max(peak, axis=1, keepdims=True)
    viol = jnp.sum(viol, axis=1, keepdims=True)
    mass = jnp.sum(mass, axis=1, keepdims=True)
    mine = jnp.where(lane == 0, peak, jnp.where(lane == 1, viol, mass))
    sown[...] = mine

    def s_copy(k):
        return pltpu.make_async_remote_copy(
            sown, srecv.at[k - 1], s_send.at[k - 1], s_recv.at[k - 1],
            device_id=(s, lax.rem(f + k, F)), device_id_type=MESH)

    for k in range(1, F):
        s_copy(k).start()

    for c in range(C * V):
        for k in range(1, A):
            y_copy(c, k).wait_send()
            ay_copy(c, k).wait_send()
        for k in range(1, B):
            z_copy(c, k).wait_send()
            az_copy(c, k).wait_send()

    def drain(t, carry):
        c_copy(t).wait_send()
        for k in range(1, X):
            x_copy(t, k).wait_send()
        out_copy(t).wait()
        return carry

    lax.fori_loop(0, T, drain, 0)
    top, add = mine, mine
    for k in range(1, F):
        s_copy(k).wait_recv()
        top = jnp.maximum(top, srecv[k - 1])
        add = add + srecv[k - 1]
    stats_out[...] = jnp.where(lane == 0, top, add / (FL * F))
    for k in range(1, F):
        s_copy(k).wait_send()


def body(S, F, design, coefficients, response, active_set, lambda_path, lambda_index):
    SL, FL = design.shape
    R = coefficients.shape[0]
    rs = lambda_path.shape[0]
    A = 1
    while (2 * A) ** 2 <= F:
        A *= 2
    B = F // A
    X = S // 2
    rf = R // F
    rp = -(-rf // 8) * 8
    Rp = F * rp
    C, T, W = SL // CHUNK, FL // TILE, SL // WIDE
    cfg = (S, F, A, B, X, R, rf, rp, rs, SL, FL)
    hbm = pl.BlockSpec(memory_space=pl.ANY)
    vmem = pl.BlockSpec(memory_space=pltpu.VMEM)
    dma = pltpu.SemaphoreType.DMA
    margins, stats = pl.pallas_call(
        functools.partial(kernel, cfg),
        out_shape=(
            jax.ShapeDtypeStruct((rs, FL), F32),
            jax.ShapeDtypeStruct((rs, 128), F32),
        ),
        in_specs=[hbm] * 6,
        out_specs=(hbm, vmem),
        scratch_shapes=[
            [pltpu.VMEM((CHUNK, FL), BF16)] * (2 * C),
            pltpu.VMEM((2 * Rp, FL), BF16),
            pltpu.VMEM((SLOTS, PIECE, FL), F32),
            pltpu.VMEM((2, CROWS, FL // 2), F32),
            pltpu.VMEM((2, CROWS, FL // 2), jnp.int32),
            pltpu.VMEM((T, 2, X, rs, TILE), F32),
            pltpu.VMEM((T, X, rs, TILE), F32),
            pltpu.VMEM((T, max(X - 1, 1), rs, TILE), F32),
            pltpu.VMEM((rs, FL), jnp.int32),
            pltpu.VMEM(lambda_path.shape, F32),
            pltpu.VMEM((1, rs), jnp.int32),
            pltpu.VMEM((W, A, B, rp, WIDE), F32),
            pltpu.VMEM((W, A - 1, B, rp, WIDE), F32),
            pltpu.VMEM((W, B, rp, WIDE), F32),
            pltpu.VMEM((W, B - 1, rp, WIDE), F32),
            pltpu.VMEM((W, A, B, rp, WIDE), F32),
            pltpu.VMEM((R, SL), F32),
            pltpu.VMEM((2 * Rp, SL), BF16),
            pltpu.VMEM((rs, 128), F32),
            pltpu.VMEM((F - 1, rs, 128), F32),
            dma((SLOTS,)), dma((2,)), dma((2,)), dma, dma, dma, dma, dma((T,)),
            dma((W, A - 1)), dma((W, A - 1)), dma((W, B - 1)), dma((W, B - 1)),
            dma((W, B - 1)), dma((W, B - 1)), dma((W, A - 1)), dma((W, A - 1)),
            dma((T,)), dma((T,)), dma((T, X - 1)), dma((T, X - 1)),
            dma((F - 1,)), dma((F - 1,)),
        ],
        compiler_params=pltpu.CompilerParams(
            collective_id=0, has_side_effects=True, vmem_limit_bytes=67043328
        ),
    )(
        design, coefficients, active_set, response, lambda_path,
        lambda_index.reshape(1, rs),
    )
    return margins, stats[:, 0], stats[:, 1], stats[:, 2]


def solution(mesh):
    return jax.shard_map(
        functools.partial(body, mesh.shape["samp"], mesh.shape["feat"]),
        mesh=mesh,
        in_specs=(
            P("samp", "feat"),
            P(None, "feat"),
            P(None, "samp"),
            P(None, "feat"),
            P("samp", None),
            P("samp"),
        ),
        out_specs=(P("samp", "feat"), P("samp"), P("samp"), P("samp")),
        check_vma=False,
    )
```
